32 devices in a mesh: section: 2 (over y), row: 4 (over z), col: 4 (over x, core).
Axes of the slice: x: 2, y: 2, z: 4, core: 2. Of those that a mesh axis runs over, the one named last changes fastest.
Arguments:
- tokens: bfloat16 [2, 256, 6144], P(None, 'col', 'row'), may hold values from -6 to 6
- ln_gain: float32 [2, 6144], P('section', 'row'), may hold values from 0.1 to 1.9
- w_query: bfloat16 [2, 6144, 6144], P('section', 'row', 'col'), as said below
- w_key: bfloat16 [2, 6144, 6144], P('section', 'row', 'col'), as said below
- w_value: bfloat16 [2, 6144, 6144], P('section', 'row', 'col'), may hold values from -0.078125 to 0.078125
- w_up: bfloat16 [2, 6144, 24576], P('section', 'row', 'col'), may hold values from -0.078125 to 0.078125
- w_out: bfloat16 [2, 6144, 6144], P('section', 'col', 'row'), may hold values from -0.078125 to 0.078125
- w_down: bfloat16 [2, 24576, 6144], P('section', 'col', 'row'), may hold values from -0.0390625 to 0.0390625
Outputs:
- section_out: bfloat16 [2, 2, 256, 6144], P('section', None, 'col', 'row')
The draws below stay inside these ranges and needn't reach their ends.
Inputs may be any that keep to these rules, and one draw needn't show every extreme that they name: `w_query`: entries are normal with standard deviation 6144 ** -0.5, clipped at six deviations. `w_key`: entries are of the order of 6144 ** -0.5; in some heads the key columns may be up to twenty times larger and correlated with the query columns.
All inputs are finite; a program needn't handle non-finite values.
Results may differ from the reference program's by a relative error of at most 0.02.
Values may be sent and summed in bfloat16 or wider, within the bound.
A program may use at most 128 MiB of HBM per device.

```python
import jax
import jax.numpy as jnp
from jax import lax

D = 6144
HEADS = 48
MLP = 24576
PATCHES = 256
IMAGES = 2
LAYERS = 2
N_ROW = 4


def base_query(key):
    values = jax.random.normal(jax.random.fold_in(key, 101), (LAYERS, D, D), jnp.float32)
    return jnp.clip(values, -6.0, 6.0) * D ** (-0.5)


def draw_w_query(key, part):
    return base_query(key).astype(jnp.bfloat16)


def draw_w_key(key, part):
    fresh = jax.random.normal(jax.random.fold_in(key, 202), (LAYERS, D, D), jnp.float32)
    fresh = jnp.clip(fresh, -6.0, 6.0) * D ** (-0.5)
    return fresh.astype(jnp.bfloat16)


def level_of(key, dims, split, low, high):
    factor_of, own = 1.0, jax.random.fold_in(key, 6)
    for dim, parts in split:
        heights = jnp.exp(jax.random.uniform(jax.random.fold_in(own, dim), (parts,), jnp.float32, low / len(split), high / len(split)))
        factor_of = factor_of * jnp.repeat(heights, dims[dim] // parts).reshape([-1 if axis == dim else 1 for axis in range(len(dims))])
    return factor_of


def bell_draw(stream_key, extent, spread, reach, cuts=(), dtype=jnp.bfloat16):
    values = spread * jax.random.normal(stream_key, extent, jnp.float32)
    if cuts:
        values = values * level_of(stream_key, extent, cuts, -0.22, 0.18)
    return jnp.clip(values, -reach, reach).astype(dtype)


def setup_inputs(seed: int = 0) -> dict:
    keys = jax.random.split(jax.random.key(seed), 9)
    tokens = bell_draw(keys[0], (IMAGES, PATCHES, D), 1.0, 6.0, ((1, 4), (2, 4)))
    ln_gain = jnp.clip(1.0 + 0.18 * jax.random.normal(keys[1], (LAYERS, D), jnp.float32), 0.1, 1.9)
    w_query = draw_w_query(jax.random.fold_in(keys[8], 71), 0)
    w_key = draw_w_key(jax.random.fold_in(keys[8], 71), 0)
    w_value = bell_draw(keys[4], (LAYERS, D, D), D ** -0.5, 0.078125, ((0, 2), (1, 4), (2, 4)))
    w_up = bell_draw(keys[5], (LAYERS, D, MLP), D ** -0.5, 0.078125, ((0, 2), (1, 4), (2, 4)))
    w_out = bell_draw(keys[6], (LAYERS, D, D), D ** -0.5, 0.078125, ((0, 2), (1, 4), (2, 4)))
    w_down = bell_draw(keys[7], (LAYERS, MLP, D), MLP ** -0.5, 0.0390625, ((0, 2), (1, 4), (2, 4)))
    return dict(tokens=tokens, ln_gain=ln_gain, w_query=w_query, w_key=w_key, w_value=w_value, w_up=w_up, w_out=w_out, w_down=w_down)


EPS = 1e-06

def project(normed, weight):
    block_width = D // N_ROW
    total = jnp.zeros((normed.shape[0], normed.shape[1], weight.shape[1]), jnp.float32)
    for block in range(N_ROW):
        part = jnp.dot(normed[:, :, block * block_width:(block + 1) * block_width], weight[block * block_width:(block + 1) * block_width], preferred_element_type=jnp.float32)
        total = total + lax.optimization_barrier(part.astype(jnp.bfloat16)).astype(jnp.float32)
    return total

def layer(x, gain, wq, wk, wv, wup, wout, wdown):
    xf = x.astype(jnp.float32)
    mean = lax.optimization_barrier(jnp.mean(xf, axis=-1, keepdims=True))
    var = jnp.maximum(lax.optimization_barrier(jnp.mean(xf * xf, axis=-1, keepdims=True)) - mean * mean, 0.0)
    normed = ((xf - mean) * lax.rsqrt(var + EPS) * gain.astype(jnp.float32)).astype(jnp.bfloat16)
    query = project(normed, wq).astype(jnp.bfloat16)
    keyed = project(normed, wk).astype(jnp.bfloat16)
    valued = project(normed, wv).astype(jnp.bfloat16)
    act = jax.nn.gelu(project(normed, wup), approximate=False).astype(jnp.bfloat16)
    head_dim = D // HEADS
    shape = (x.shape[0], x.shape[1], HEADS, head_dim)
    qh = query.reshape(shape).astype(jnp.float32)
    kh = keyed.reshape(shape).astype(jnp.float32)
    vh = valued.reshape(shape).astype(jnp.float32)
    scores = jnp.einsum('bqhd,bkhd->bhqk', qh, kh) / jnp.sqrt(jnp.float32(head_dim))
    scores = scores - lax.optimization_barrier(jnp.max(scores, axis=-1, keepdims=True))
    weights = jnp.exp(scores)
    probs = (weights / lax.optimization_barrier(jnp.sum(weights, axis=-1, keepdims=True))).astype(jnp.bfloat16)
    attn = jnp.einsum('bhqk,bkhd->bqhd', probs.astype(jnp.float32), vh)
    attn = attn.reshape(x.shape).astype(jnp.bfloat16)
    mixed = jnp.dot(attn, wout, preferred_element_type=jnp.float32) + jnp.dot(act, wdown, preferred_element_type=jnp.float32)
    return (xf + mixed).astype(jnp.bfloat16)

def reference(tokens, ln_gain, w_query, w_key, w_value, w_up, w_out, w_down):
    current = tokens
    outputs = []
    for level in range(LAYERS):
        current = layer(current, ln_gain[level], w_query[level], w_key[level], w_value[level], w_up[level], w_out[level], w_down[level])
        outputs.append(current)
    return jnp.stack(outputs)
```

```python
import functools
from typing import NamedTuple

import jax
import jax.numpy as jnp
from jax import lax
from jax.experimental import pallas as pl
from jax.experimental.pallas import tpu as pltpu
from jax.sharding import PartitionSpec as P

D = 6144
HEADS = 48
HEAD = D // HEADS


EPS = 1e-06
MESH = pl.DeviceIdType.MESH
VMEM_BYTES = 60 * 1024 * 1024
LAG = 2
RUNG = 2
SLOTS = 3
PAIR_LAG = 2
CROSS_LAG = 5


class Plan(NamedTuple):
    owner: int
    last: bool
    rows: int
    cols: int
    images: int
    heads: tuple
    units: tuple

    def chunks(self, half):
        return 3 * self.heads[half] + self.units[half]


def plan_of(x, wq, wup, owner, last):
    heads = wq.shape[1] // HEAD // 2
    units = wup.shape[1] // HEAD // 2
    far_heads = heads // 2
    far_units = units * 5 // 12
    return Plan(
        owner,
        last,
        lax.axis_size("row"),
        lax.axis_size("col"),
        x.shape[0],
        (heads - far_heads, far_heads),
        (units - far_units, far_units),
    )


def greet_peers(axes):
    barrier = pltpu.get_barrier_semaphore()
    total = 0
    for axis, count in axes:
        me = lax.axis_index(axis)
        for step in range(1, count):
            pl.semaphore_signal(
                barrier, inc=1, device_id={axis: lax.rem(me + step, count)}, device_id_type=MESH
            )
            total += 1
    pl.semaphore_wait(barrier, total)


def both(first, *rest):
    for other in rest:
        first = jnp.logical_and(first, other)
    return first


def layer_kernel(
    plan,
    x_ref,
    gain_ref,
    wq_ref,
    wk_ref,
    wv_ref,
    wup_ref,
    wout_ref,
    wdown_ref,
    out_ref,
    stats,
    full,
    part,
    away,
    held,
    act,
    far,
    wbuf,
    dbuf,
    acc,
    own,
    pair_out,
    pair_in,
    cross_out,
    cross_in,
    stat_sem,
    gather_sem,
    wsem,
    dsem,
    reduce_sem,
    spread_sem,
    rung_sem,
    far_sem,
    pair_sem,
    cross_sem,
    pass_sem,
):
    rows, cols, images = plan.rows, plan.cols, plan.images
    last = rows - 1
    per_image = max(plan.chunks(0), plan.chunks(1))
    count = images * per_image
    row, col, section = lax.axis_index("row"), lax.axis_index("col"), lax.axis_index("section")
    is_owner = section == plan.owner
    is_far = jnp.logical_not(is_owner)
    chips = cols // 2
    chip, core = lax.div(col, 2), lax.rem(col, 2)
    partner = 2 * chip + (1 - core)
    patches, width = x_ref.shape[1], x_ref.shape[2]
    total_rows = patches * cols
    entry = jnp.where(is_owner, 0, RUNG)
    my_heads = jnp.where(is_owner, plan.heads[0], plan.heads[1])
    my_chunks = jnp.where(is_owner, plan.chunks(0), plan.chunks(1))
    depth = 2 * RUNG + 2 * LAG * last
    greet_peers((("row", rows), ("col", cols), ("section", 2)))

    def remote(src, dst, send, recv, **where):
        return pltpu.make_async_remote_copy(
            src_ref=src, dst_ref=dst, send_sem=send, recv_sem=recv, device_id=where, device_id_type=MESH
        )

    def chip_at(step):
        return lax.rem(chip + step, chips)

    def chip_behind(step):
        return lax.rem(chip + chips - step, chips)

    def gather_cross(image, step):
        place = full.at[image, col]
        return remote(
            place,
            place,
            gather_sem.at[0, 0, image, step],
            gather_sem.at[0, 1, image, step],
            col=2 * chip_at(step) + core,
        )

    def gather_pair(image, step):
        place = full.at[image, 2 * chip_behind(step) + core]
        return remote(
            place, place, gather_sem.at[1, 0, image, step], gather_sem.at[1, 1, image, step], col=partner
        )

    def relay(image):
        for step in range(1, chips):
            gather_cross(image, step).wait_recv()
            gather_pair(image, step).start()

    def gathered(image):
        for step in range(chips):
            gather_pair(image, step).wait_recv()

    def chunk_kind(half, j):
        heads = 3 * plan.heads[half]
        return j < heads, lax.rem(j, 3), lax.div(j, 3), j - heads

    def head_base(half, side):
        return side * plan.heads[0] if half == 0 else 2 * plan.heads[0] + side * plan.heads[1]

    def unit_base(half, side):
        return side * plan.units[0] if half == 0 else 2 * plan.units[0] + side * plan.units[1]

    def in_copy(ref, half, side, slot, block):
        start = pl.multiple_of(block * HEAD, HEAD)
        return pltpu.make_async_copy(
            ref.at[:, pl.ds(start, HEAD)],
            wbuf.at[slot, half, :, pl.ds(side * HEAD, HEAD)],
            wsem.at[slot, half, side],
        )

    def out_copy(ref, half, side, slot, block):
        start = pl.multiple_of(block * HEAD, HEAD)
        return pltpu.make_async_copy(
            ref.at[pl.ds(start, HEAD), :],
            dbuf.at[slot, half, pl.ds(side * HEAD, HEAD), :],
            dsem.at[slot, half, side],
        )

    def fetch_in(c):
        j, slot = lax.rem(c, per_image), lax.rem(c, SLOTS)
        for half in range(2):
            is_head, kind, head, unit = chunk_kind(half, j)
            for index, ref in enumerate((wq_ref, wk_ref, wv_ref)):

                @pl.when(both(is_head, kind == index))
                def _():
                    for side in range(2):
                        in_copy(ref, half, side, slot, head_base(half, side) + head).start()

            @pl.when(both(jnp.logical_not(is_head), j < plan.chunks(half)))
            def _():
                for side in range(2):
                    in_copy(wup_ref, half, side, slot, unit_base(half, side) + unit).start()

    def yields(half, j):
        is_head, kind, _, _ = chunk_kind(half, j)
        return jnp.logical_or(both(is_head, kind == 2), both(jnp.logical_not(is_head), j < plan.chunks(half)))

    def fetch_out(c):
        j, slot = lax.rem(c, per_image), lax.rem(c, SLOTS)
        for half in range(2):
            is_head, kind, head, unit = chunk_kind(half, j)

            @pl.when(both(is_head, kind == 2))
            def _():
                for side in range(2):
                    out_copy(wout_ref, half, side, slot, head_base(half, side) + head).start()

            @pl.when(both(jnp.logical_not(is_head), j < plan.chunks(half)))
            def _():
                for side in range(2):
                    out_copy(wdown_ref, half, side, slot, unit_base(half, side) + unit).start()

    def rung_copy(c):
        return remote(away.at[c], part.at[c], rung_sem.at[0, c], rung_sem.at[1, c], section=1 - section)

    def far_copy(side, c):
        return remote(
            act.at[side, c],
            far.at[side, c],
            far_sem.at[0, side, c],
            far_sem.at[1, side, c],
            section=1 - section,
        )

    def toward(side):
        return jnp.minimum(row + 1, last) if side == 1 else jnp.maximum(row - 1, 0)

    def hops_of(side):
        return row if side == 1 else last - row

    def reduce_copy(side, c, own_part):
        src = part.at[c, side] if own_part else held.at[side, c]
        return remote(
            src, held.at[side, c], reduce_sem.at[0, side, c], reduce_sem.at[1, side, c], row=toward(side)
        )

    def spread_copy(side, c):
        place = act.at[side, c]
        return remote(
            place, place, spread_sem.at[0, side, c], spread_sem.at[1, side, c], row=toward(1 - side)
        )

    def project(c):
        image, j, slot = lax.div(c, per_image), lax.rem(c, per_image), lax.rem(c, SLOTS)
        for half in range(2):

            @pl.when(j < plan.chunks(half))
            def _():
                for side in range(2):
                    in_copy(wup_ref, half, side, slot, 0).wait()
                value = jnp.dot(
                    full[image].reshape(total_rows, width),
                    wbuf[slot, half],
                    preferred_element_type=jnp.float32,
                ).astype(jnp.bfloat16)
                target = part if half == 0 else away
                target[c, 0] = value[:, :HEAD]
                target[c, 1] = value[:, HEAD:]

        @pl.when(j < plan.chunks(1))
        def _():
            rung_copy(c).start()

        @pl.when(c + SLOTS < count)
        def _():
            fetch_in(c + SLOTS)

    def attend(side, c, value):
        scores = lax.dot_general(
            held[side, c - 2], held[side, c - 1], (((1,), (1,)), ((), ())), preferred_element_type=jnp.float32
        ) / (float(HEAD) ** 0.5)
        expo = jnp.exp(scores - jnp.max(scores, axis=-1, keepdims=True))
        probs = (expo / jnp.sum(expo, axis=-1, keepdims=True)).astype(jnp.bfloat16)
        return jnp.dot(probs, value, preferred_element_type=jnp.float32).astype(jnp.bfloat16)

    def finish_sum(side, c, j):
        total = part[c, side].astype(jnp.float32) + held[side, c].astype(jnp.float32)
        is_head, kind = j < 3 * my_heads, lax.rem(j, 3)

        @pl.when(is_head)
        def _():
            held[side, c] = total.astype(jnp.bfloat16)

        @pl.when(both(is_head, kind == 2))
        def _():
            act[side, c] = attend(side, c, total.astype(jnp.bfloat16))

        @pl.when(jnp.logical_not(is_head))
        def _():
            act[side, c] = (0.5 * total * (1.0 + lax.erf(total * (0.5**0.5)))).astype(jnp.bfloat16)

    def my_yield(j):
        is_head, kind = j < 3 * my_heads, lax.rem(j, 3)
        return jnp.logical_or(both(is_head, kind == 2), both(jnp.logical_not(is_head), j < my_chunks))

    def in_range(c):
        return both(c >= 0, c < count)

    def spread_stage(s):
        for side in range(2):
            dist = hops_of(1 - side)
            c = s - entry - LAG * (last + dist)
            j = lax.rem(c, per_image)

            @pl.when(both(dist > 0, in_range(c), my_yield(j)))
            def _():
                spread_copy(side, c).wait_recv()

                @pl.when(dist < last)
                def _():
                    spread_copy(side, c).start()

                @pl.when(is_far)
                def _():
                    far_copy(side, c).start()

    def reduce_stage(s):
        c_rung = s - RUNG

        @pl.when(both(is_far, in_range(c_rung), lax.rem(c_rung, per_image) < plan.chunks(1)))
        def _():
            rung_copy(c_rung).wait_recv()

        for side in range(2):
            hops = hops_of(side)
            c = s - entry - LAG * hops
            live = both(in_range(c), lax.rem(c, per_image) < my_chunks)

            @pl.when(both(live, hops == 0))
            def _():
                reduce_copy(side, c, True).start()

            @pl.when(both(live, hops > 0, hops < last))
            def _():
                reduce_copy(side, c, False).wait_recv()
                held[side, c] = (
                    part[c, side].astype(jnp.float32) + held[side, c].astype(jnp.float32)
                ).astype(jnp.bfloat16)
                reduce_copy(side, c, False).start()

    def root_stage(s):
        side = jnp.where(row == 0, 0, 1)
        c = s - entry - LAG * last
        j = lax.rem(c, per_image)

        @pl.when(both(jnp.logical_or(row == 0, row == last), in_range(c), j < my_chunks))
        def _():
            for which in range(2):

                @pl.when(side == which)
                def _():
                    reduce_copy(which, c, False).wait_recv()

            finish_sum(side, c, j)

            @pl.when(my_yield(j))
            def _():
                for which in range(2):

                    @pl.when(side == which)
                    def _():
                        spread_copy(which, c).start()

                        @pl.when(is_far)
                        def _():
                            far_copy(which, c).start()

    def down_stage(s):
        c = s - depth

        @pl.when(in_range(c))
        def _():
            j, slot = lax.rem(c, per_image), lax.rem(c, SLOTS)

            @pl.when(j == 0)
            def _():
                acc[...] = jnp.zeros_like(acc)

            for half in range(2):

                @pl.when(yields(half, j))
                def _():
                    source = act if half == 0 else far
                    for side in range(2):
                        if half == 1:
                            far_copy(side, c).wait_recv()
                        out_copy(wdown_ref, half, side, slot, 0).wait()
                    lhs = jnp.concatenate([source[0, c], source[1, c]], axis=1)
                    acc[...] += jnp.dot(lhs, dbuf[slot, half], preferred_element_type=jnp.float32).reshape(
                        acc.shape
                    )

            @pl.when(c + SLOTS < count)
            def _():
                fetch_out(c + SLOTS)

    def pair_copy(image):
        return remote(
            pair_out.at[image], pair_in.at[image], pair_sem.at[0, image], pair_sem.at[1, image], col=partner
        )

    def cross_copy(image, step):
        return remote(
            cross_out.at[image, step],
            cross_in.at[image, step],
            cross_sem.at[0, image, step],
            cross_sem.at[1, image, step],
            col=2 * chip_at(step) + core,
        )

    def pass_copy(image):
        return remote(
            out_ref.at[image],
            out_ref.at[image],
            pass_sem.at[0, image],
            pass_sem.at[1, image],
            section=1 - section,
        )

    def ended(s, lag):
        done = s - depth - lag + 1
        return both(done > 0, done <= count, lax.rem(done, per_image) == 0), lax.div(done, per_image) - 1

    def close_stage(s):
        at_end, image = ended(s, 0)

        @pl.when(at_end)
        def _():
            for step in range(chips):
                theirs = 2 * chip_at(step)
                pair_out[image, step] = acc[theirs + (1 - core)].astype(jnp.bfloat16)
                own[step] = acc[theirs + core]
            pair_copy(image).start()

        at_pair, image_pair = ended(s, PAIR_LAG)

        @pl.when(at_pair)
        def _():
            pair_copy(image_pair).wait_recv()
            for step in range(1, chips):
                cross_out[image_pair, step] = (
                    own[step] + pair_in[image_pair, step].astype(jnp.float32)
                ).astype(jnp.bfloat16)
                cross_copy(image_pair, step).start()
            own[0] = own[0] + pair_in[image_pair, 0].astype(jnp.float32)

        at_cross, image_cross = ended(s, PAIR_LAG + CROSS_LAG)

        @pl.when(at_cross)
        def _():
            total = own[0]
            for step in range(1, chips):
                cross_copy(image_cross, step).wait_recv()
                total = total + cross_in[image_cross, step].astype(jnp.float32)
            out_ref[image_cross] = (x_ref[image_cross].astype(jnp.float32) + total).astype(jnp.bfloat16)
            if not plan.last:
                pass_copy(image_cross).start()

    @pl.when(is_owner)
    def _():
        for c in range(SLOTS):
            fetch_in(jnp.int32(c))
            fetch_out(jnp.int32(c))
        xf = x_ref[...].reshape(images * patches, width).astype(jnp.float32)
        total = jnp.sum(xf, axis=-1, keepdims=True)
        square = jnp.sum(xf * xf, axis=-1, keepdims=True)
        lane = lax.broadcasted_iota(jnp.int32, (images * patches, 128), 1)
        stats[0] = jnp.where(lane < 64, total, square)
        copies = []
        for step in range(1, rows):
            copy = remote(
                stats.at[0],
                stats.at[step],
                stat_sem.at[0, step],
                stat_sem.at[1, step],
                row=lax.rem(row + step, rows),
            )
            copy.start()
            copies.append(copy)
        for copy in copies:
            copy.wait()
        sums = stats[0]
        for step in range(1, rows):
            sums = sums + stats[step]
        mean = sums[:, 0:1] / D
        var = jnp.maximum(sums[:, 64:65] / D - mean * mean, 0.0)
        normed = ((xf - mean) * lax.rsqrt(var + EPS) * gain_ref[...]).astype(jnp.bfloat16)
        for image in range(images):
            full[image, col] = normed[image * patches : (image + 1) * patches]
            for step in range(1, chips):
                gather_cross(image, step).start()
            gather_pair(image, 0).start()
        relay(0)
        gathered(0)
        project(jnp.int32(0))

    def step(s, carry):
        spread_stage(s)
        reduce_stage(s)
        root_stage(s)

        @pl.when(is_owner)
        def _():
            for image in range(1, images):

                @pl.when(s == image * per_image - per_image // 2)
                def _():
                    relay(image)

                @pl.when(s == image * per_image - 1)
                def _():
                    gathered(image)

            @pl.when(s + 1 < count)
            def _():
                project(s + 1)

            down_stage(s)
            close_stage(s)

        return carry

    lax.fori_loop(0, count + depth + PAIR_LAG + CROSS_LAG, step, 0)

    def drain(c, carry):
        j = lax.rem(c, per_image)
        for side in range(2):
            hops = hops_of(side)

            @pl.when(both(j < my_chunks, hops < last))
            def _():
                reduce_copy(side, c, False).wait_send()

            @pl.when(my_yield(j))
            def _():
                @pl.when(hops_of(1 - side) < last)
                def _():
                    spread_copy(side, c).wait_send()

                @pl.when(is_far)
                def _():
                    far_copy(side, c).wait_send()

        @pl.when(both(is_owner, j < plan.chunks(1)))
        def _():
            rung_copy(c).wait_send()

        return carry

    lax.fori_loop(0, count, drain, 0)

    @pl.when(is_owner)
    def _():
        for image in range(images):
            for step in range(chips):
                gather_pair(image, step).wait_send()
                if step:
                    gather_cross(image, step).wait_send()
                    cross_copy(image, step).wait_send()
            pair_copy(image).wait_send()
            if not plan.last:
                pass_copy(image).wait_send()

    if not plan.last:

        @pl.when(is_far)
        def _():
            for image in range(images):
                pass_copy(image).wait_recv()


def fused_layer(x, weights, owner, last):
    gain, wq, wk, wv, wup, wout, wdown = weights
    plan = plan_of(x, wq, wup, owner, last)
    images, patches, width = x.shape
    rows, cols = plan.rows, plan.cols
    chips = cols // 2
    count = images * max(plan.chunks(0), plan.chunks(1))
    total_rows = patches * cols
    bf16, f32 = jnp.bfloat16, jnp.float32
    dma = pltpu.SemaphoreType.DMA
    vmem = pl.BlockSpec(memory_space=pltpu.VMEM)
    hbm = pl.BlockSpec(memory_space=pl.ANY)
    return pl.pallas_call(
        functools.partial(layer_kernel, plan),
        out_shape=jax.ShapeDtypeStruct(x.shape, bf16),
        in_specs=[vmem, vmem] + [hbm] * 6,
        out_specs=vmem,
        scratch_shapes=[
            pltpu.VMEM((rows, images * patches, 128), f32),
            pltpu.VMEM((images, cols, patches, width), bf16),
            pltpu.VMEM((count, 2, total_rows, HEAD), bf16),
            pltpu.VMEM((count, 2, total_rows, HEAD), bf16),
            pltpu.VMEM((2, count, total_rows, HEAD), bf16),
            pltpu.VMEM((2, count, total_rows, HEAD), bf16),
            pltpu.VMEM((2, count, total_rows, HEAD), bf16),
            pltpu.VMEM((SLOTS, 2, width, 2 * HEAD), bf16),
            pltpu.VMEM((SLOTS, 2, 2 * HEAD, width), bf16),
            pltpu.VMEM((cols, patches, width), f32),
            pltpu.VMEM((chips, patches, width), f32),
            pltpu.VMEM((images, chips, patches, width), bf16),
            pltpu.VMEM((images, chips, patches, width), bf16),
            pltpu.VMEM((images, chips, patches, width), bf16),
            pltpu.VMEM((images, chips, patches, width), bf16),
            dma((2, rows)),
            dma((2, 2, images, chips)),
            dma((SLOTS, 2, 2)),
            dma((SLOTS, 2, 2)),
            dma((2, 2, count)),
            dma((2, 2, count)),
            dma((2, count)),
            dma((2, 2, count)),
            dma((2, images)),
            dma((2, images, chips)),
            dma((2, images)),
        ],
        compiler_params=pltpu.CompilerParams(
            collective_id=owner, has_side_effects=True, vmem_limit_bytes=VMEM_BYTES
        ),
    )(x, gain[None], wq, wk, wv, wup, wout, wdown)


def fits(x, wq, wup):
    rows, cols = lax.axis_size("row"), lax.axis_size("col")
    heads, units = wq.shape[1] // HEAD, wup.shape[1] // HEAD
    return (
        lax.axis_size("section") == 2
        and rows > 1
        and cols % 2 == 0
        and x.shape[1] % 16 == 0
        and wq.shape[1] % (2 * HEAD) == 0
        and wup.shape[1] % (2 * HEAD) == 0
        and heads >= 4
        and units >= 6
    )


def passed_along(value, axis, steps):
    count = lax.axis_size(axis)
    first, last = (max(0, -steps), min(count, count - steps))
    return lax.ppermute(value, axis, [(source, source + steps) for source in range(first, last)])


def layer(x, weights):
    gain, wq, wk, wv, wup, wout, wdown = weights
    xf = x.astype(jnp.float32)
    sums, squares = lax.psum((jnp.sum(xf, axis=-1), jnp.sum(xf * xf, axis=-1)), "row")
    mean = (sums / D)[..., None]
    var = jnp.maximum((squares / D)[..., None] - mean * mean, 0.0)
    normed = ((xf - mean) * lax.rsqrt(var + EPS) * gain).astype(jnp.bfloat16)
    gathered = lax.all_gather(normed, "col", axis=1, tiled=True)
    part_q = jnp.dot(gathered, wq, preferred_element_type=jnp.float32)
    part_k = jnp.dot(gathered, wk, preferred_element_type=jnp.float32)
    part_v = jnp.dot(gathered, wv, preferred_element_type=jnp.float32)
    part_m = jnp.dot(gathered, wup, preferred_element_type=jnp.float32)
    query, keyed, valued, pre = (
        lax.psum_scatter(
            part_q.astype(jnp.bfloat16), "row", scatter_dimension=1, tiled=True
        ).astype(jnp.float32),
        lax.psum_scatter(
            part_k.astype(jnp.bfloat16), "row", scatter_dimension=1, tiled=True
        ).astype(jnp.float32),
        lax.psum_scatter(
            part_v.astype(jnp.bfloat16), "row", scatter_dimension=1, tiled=True
        ).astype(jnp.float32),
        lax.psum_scatter(
            part_m.astype(jnp.bfloat16), "row", scatter_dimension=1, tiled=True
        ).astype(jnp.float32),
    )
    act = jax.nn.gelu(pre, approximate=False).astype(jnp.bfloat16)
    query = query.astype(jnp.bfloat16)
    keyed = keyed.astype(jnp.bfloat16)
    valued = valued.astype(jnp.bfloat16)
    all_keys, all_values = (
        lax.all_gather(keyed, "row", axis=1, tiled=True),
        lax.all_gather(valued, "row", axis=1, tiled=True),
    )
    head_dim = D // HEADS
    local_heads = query.shape[2] // head_dim
    images = query.shape[0]
    qh = query.reshape(images, query.shape[1], local_heads, head_dim)
    kh = all_keys.reshape(images, all_keys.shape[1], local_heads, head_dim)
    vh = all_values.reshape(images, all_values.shape[1], local_heads, head_dim)
    scores = jnp.einsum("bqhd,bkhd->bhqk", qh, kh, preferred_element_type=jnp.float32) / jnp.sqrt(
        jnp.float32(head_dim)
    )
    scores = scores - jnp.max(scores, axis=-1, keepdims=True)
    expo = jnp.exp(scores)
    probs = (expo / jnp.sum(expo, axis=-1, keepdims=True)).astype(jnp.bfloat16)
    attn = jnp.einsum("bhqk,bkhd->bqhd", probs, vh, preferred_element_type=jnp.float32)
    attn = attn.reshape(query.shape).astype(jnp.bfloat16)
    attn_full, act_full = (
        lax.all_gather(attn, "row", axis=1, tiled=True),
        lax.all_gather(act, "row", axis=1, tiled=True),
    )
    mixed = jnp.dot(attn_full, wout, preferred_element_type=jnp.float32) + jnp.dot(
        act_full, wdown, preferred_element_type=jnp.float32
    )
    summed = lax.psum_scatter(
        mixed.astype(jnp.bfloat16), "col", scatter_dimension=1, tiled=True
    ).astype(jnp.float32)
    return (xf + summed).astype(jnp.bfloat16)


def pass_on(output):
    return passed_along(output, "section", 1)


def local(tokens, ln_gain, w_query, w_key, w_value, w_up, w_out, w_down):
    weights = (ln_gain[0], w_query[0], w_key[0], w_value[0], w_up[0], w_out[0], w_down[0])
    section = lax.axis_index("section")
    sections = lax.axis_size("section")
    if fits(tokens, w_query[0], w_up[0]):
        first = fused_layer(tokens, weights, 0, False)
        second = fused_layer(first, weights, 1, True)
        return jnp.where(section == 0, first, second)[None]
    result = jnp.zeros_like(tokens)
    images = tokens.shape[0]
    ticks = images + sections - 1
    inbox = jnp.zeros_like(tokens[:1])
    positions = jnp.arange(images, dtype=jnp.int32)
    for tick in range(ticks):
        fresh = tokens[min(tick, images - 1) : min(tick, images - 1) + 1]
        current = jnp.where(section == 0, fresh, inbox)
        output = layer(current, weights)
        slot = tick - section
        result = jnp.where((positions == slot)[:, None, None], output, result)
        if tick + 1 < ticks:
            inbox = pass_on(output)
    return result[None]


def solution(mesh):
    return jax.shard_map(
        local,
        mesh=mesh,
        in_specs=(
            P(None, "col", "row"),
            P("section", "row"),
            P("section", "row", "col"),
            P("section", "row", "col"),
            P("section", "row", "col"),
            P("section", "row", "col"),
            P("section", "col", "row"),
            P("section", "col", "row"),
        ),
        out_specs=P("section", None, "col", "row"),
        check_vma=False,
    )
```

```python
import functools
from typing import NamedTuple

import jax
import jax.numpy as jnp
from jax import lax
from jax.experimental import pallas as pl
from jax.experimental.pallas import tpu as pltpu
from jax.sharding import PartitionSpec as P

D = 6144
HEADS = 48
HEAD = D // HEADS


EPS = 1e-06
MESH = pl.DeviceIdType.MESH
VMEM_BYTES = 67043328
LAG = 2
RUNG = 2
SLOTS = 3
PAIR_LAG = 2
CROSS_LAG = 3
PASS_LAG = 2
STAT_LAG = 2
RELAY_LAG = 2
GATHER_LAG = 1


class Plan(NamedTuple):
    rows: int
    cols: int
    images: int
    heads: tuple
    units: tuple

    def slots(self):
        return 3 * self.heads[0] + self.units[0]

    def group(self):
        return -(-self.slots() // self.heads[0])

    def quota(self, half):
        return -(-self.units[1] // self.heads[0]) if half else self.group() - 3

    def kind(self, half, j):
        group, pos = lax.div(j, self.group()), lax.rem(j, self.group())
        unit = group * self.quota(half) + pos - 3
        is_head = both(pos < 3, group < self.heads[half])
        is_unit = both(pos >= 3, pos < 3 + self.quota(half), unit < self.units[half])
        return is_head, is_unit, pos, group, unit, group * (3 + self.quota(half)) + pos

    def used(self):
        groups, quota = self.heads[0], self.quota(1)
        used = [(g, p) for g in range(self.heads[1]) for p in range(3)]
        used += [(u // quota, 3 + u % quota) for u in range(self.units[1])]
        return max(g * self.group() + p for g, p in used), max(g * (3 + quota) + p for g, p in used)


def plan_of(x, wq, wup):
    heads = wq.shape[1] // HEAD // 2
    units = wup.shape[1] // HEAD // 2
    far_heads = heads // 2
    far_units = units * 5 // 12
    return Plan(
        lax.axis_size("row"),
        lax.axis_size("col"),
        x.shape[0],
        (heads - far_heads, far_heads),
        (units - far_units, far_units),
    )


def greet_peers(axes):
    barrier = pltpu.get_barrier_semaphore()
    total = 0
    for axis, count in axes:
        me = lax.axis_index(axis)
        for step in range(1, count):
            pl.semaphore_signal(
                barrier, inc=1, device_id={axis: lax.rem(me + step, count)}, device_id_type=MESH
            )
            total += 1
    pl.semaphore_wait(barrier, total)


def both(first, *rest):
    for other in rest:
        first = jnp.logical_and(first, other)
    return first


def layers_kernel(
    plan,
    x_ref,
    gain_ref,
    wq_ref,
    wk_ref,
    wv_ref,
    wup_ref,
    wout_ref,
    wdown_ref,
    out_ref,
    inbox,
    stats,
    full,
    part_near,
    part_far,
    held_near,
    held_far,
    act_near,
    act_far,
    away,
    back,
    wbuf,
    dbuf,
    acc,
    pair_out,
    pair_in,
    cross_out,
    cross_in,
    stat_sem,
    gather_sem,
    wsem,
    dsem,
    reduce_near,
    reduce_far,
    spread_near,
    spread_far,
    rung_sem,
    back_sem,
    pair_sem,
    cross_sem,
    pass_sem,
):
    rows, cols, images = plan.rows, plan.cols, plan.images
    last = rows - 1
    per_image, per_far = plan.slots(), plan.used()[1] + 1
    count = images * per_image
    row, col, section = lax.axis_index("row"), lax.axis_index("col"), lax.axis_index("section")
    chips = cols // 2
    chip, core = lax.div(col, 2), lax.rem(col, 2)
    partner = 2 * chip + (1 - core)
    patches, width = x_ref.shape[1], x_ref.shape[2]
    total_rows = patches * cols
    line = 2 * LAG * last
    closing = max(per_image - 1, plan.used()[0] + 2 * RUNG) + line
    passed = closing + PAIR_LAG + CROSS_LAG
    arrive = passed + PASS_LAG
    second = arrive + STAT_LAG + RELAY_LAG + GATHER_LAG + 1
    base = (section * second, (1 - section) * second)
    entry = (0, RUNG)
    parts, helds, acts = (part_near, part_far), (held_near, held_far), (act_near, act_far)
    reduce_sems, spread_sems = (reduce_near, reduce_far), (spread_near, spread_far)
    greet_peers((("row", rows), ("col", cols), ("section", 2)))

    def remote(src, dst, send, recv, **where):
        return pltpu.make_async_remote_copy(
            src_ref=src, dst_ref=dst, send_sem=send, recv_sem=recv, device_id=where, device_id_type=MESH
        )

    def split(c):
        return lax.div(c, per_image), lax.rem(c, per_image)

    def far_place(c):
        image, j = split(c)
        return image * per_far + plan.kind(1, j)[5]

    def place_of(role, c):
        return c if role == 0 else far_place(c)

    def in_range(c):
        return both(c >= 0, c < count)

    def used(role, j):
        is_head, is_unit = plan.kind(role, j)[:2]
        return jnp.logical_or(is_head, is_unit)

    def yields(role, j):
        is_head, is_unit, pos = plan.kind(role, j)[:3]
        return jnp.logical_or(both(is_head, pos == 2), is_unit)

    def chip_at(step):
        return lax.rem(chip + step, chips)

    def chip_behind(step):
        return lax.rem(chip + chips - step, chips)

    def gather_cross(image, step):
        place = full.at[image, col]
        return remote(
            place,
            place,
            gather_sem.at[0, 0, image, step],
            gather_sem.at[0, 1, image, step],
            col=2 * chip_at(step) + core,
        )

    def gather_pair(image, step):
        place = full.at[image, 2 * chip_behind(step) + core]
        return remote(
            place, place, gather_sem.at[1, 0, image, step], gather_sem.at[1, 1, image, step], col=partner
        )

    def stat_copy(image, step):
        return remote(
            stats.at[image, 0],
            stats.at[image, step],
            stat_sem.at[0, image, step],
            stat_sem.at[1, image, step],
            row=lax.rem(row + step, rows),
        )

    def measure(image):
        xf = inbox[image].astype(jnp.float32)
        total = jnp.sum(xf, axis=-1, keepdims=True)
        square = jnp.sum(xf * xf, axis=-1, keepdims=True)
        lane = lax.broadcasted_iota(jnp.int32, (patches, 128), 1)
        stats[image, 0] = jnp.where(lane < 64, total, square)
        for step in range(1, rows):
            stat_copy(image, step).start()

    def normalize(image):
        sums = stats[image, 0]
        for step in range(1, rows):
            stat_copy(image, step).wait_recv()
            sums = sums + stats[image, step]
        mean = sums[:, 0:1] / D
        var = jnp.maximum(sums[:, 64:65] / D - mean * mean, 0.0)
        xf = inbox[image].astype(jnp.float32)
        full[image, col] = ((xf - mean) * lax.rsqrt(var + EPS) * gain_ref[...]).astype(jnp.bfloat16)
        for step in range(1, chips):
            gather_cross(image, step).start()
        gather_pair(image, 0).start()

    def relay(image):
        for step in range(1, chips):
            gather_cross(image, step).wait_recv()
            gather_pair(image, step).start()

    def gathered(image):
        for step in range(chips):
            gather_pair(image, step).wait_recv()

    def head_base(half, side):
        return side * plan.heads[0] if half == 0 else 2 * plan.heads[0] + side * plan.heads[1]

    def unit_base(half, side):
        return side * plan.units[0] if half == 0 else 2 * plan.units[0] + side * plan.units[1]

    def in_copy(ref, half, side, slot, block):
        start = pl.multiple_of(block * HEAD, HEAD)
        return pltpu.make_async_copy(
            ref.at[:, pl.ds(start, HEAD)],
            wbuf.at[slot, half, :, pl.ds(side * HEAD, HEAD)],
            wsem.at[slot, half, side],
        )

    def out_copy(ref, half, side, slot, block):
        start = pl.multiple_of(block * HEAD, HEAD)
        return pltpu.make_async_copy(
            ref.at[pl.ds(start, HEAD), :],
            dbuf.at[slot, half, pl.ds(side * HEAD, HEAD), :],
            dsem.at[slot, half, side],
        )

    def fetch_in(c):
        _, j = split(c)
        slot = lax.rem(c, SLOTS)
        for half in range(2):
            is_head, is_unit, kind, head, unit, _ = plan.kind(half, j)
            for index, ref in enumerate((wq_ref, wk_ref, wv_ref)):

                @pl.when(both(is_head, kind == index))
                def _():
                    for side in range(2):
                        in_copy(ref, half, side, slot, head_base(half, side) + head).start()

            @pl.when(is_unit)
            def _():
                for side in range(2):
                    in_copy(wup_ref, half, side, slot, unit_base(half, side) + unit).start()

    def fetch_out(half, c):
        _, j = split(c)
        slot = lax.rem(c, SLOTS)
        is_head, is_unit, kind, head, unit, _ = plan.kind(half, j)

        @pl.when(both(is_head, kind == 2))
        def _():
            for side in range(2):
                out_copy(wout_ref, half, side, slot, head_base(half, side) + head).start()

        @pl.when(is_unit)
        def _():
            for side in range(2):
                out_copy(wdown_ref, half, side, slot, unit_base(half, side) + unit).start()

    def rung_copy(place):
        return remote(
            away.at[place], part_far.at[place], rung_sem.at[0, place], rung_sem.at[1, place], section=1 - section
        )

    def back_copy(side, place):
        return remote(
            act_far.at[side, place],
            back.at[side, place],
            back_sem.at[0, side, place],
            back_sem.at[1, side, place],
            section=1 - section,
        )

    def toward(side):
        return jnp.minimum(row + 1, last) if side == 1 else jnp.maximum(row - 1, 0)

    def hops_of(side):
        return row if side == 1 else last - row

    def reduce_copy(role, side, place, own_part):
        held, sem = helds[role], reduce_sems[role]
        src = parts[role].at[place, side] if own_part else held.at[side, place]
        return remote(
            src, held.at[side, place], sem.at[0, side, place], sem.at[1, side, place], row=toward(side)
        )

    def spread_copy(role, side, place):
        here, sem = acts[role].at[side, place], spread_sems[role]
        return remote(here, here, sem.at[0, side, place], sem.at[1, side, place], row=toward(1 - side))

    def project(c):
        image, j = split(c)
        slot = lax.rem(c, SLOTS)
        for half in range(2):

            @pl.when(used(half, j))
            def _():
                for side in range(2):
                    in_copy(wup_ref, half, side, slot, 0).wait()
                value = jnp.dot(
                    full[image].reshape(total_rows, width),
                    wbuf[slot, half],
                    preferred_element_type=jnp.float32,
                ).astype(jnp.bfloat16)
                target, place = (part_near, c) if half == 0 else (away, far_place(c))
                target[place, 0] = value[:, :HEAD]
                target[place, 1] = value[:, HEAD:]
                if half == 1:
                    rung_copy(place).start()

        @pl.when(c + SLOTS < count)
        def _():
            fetch_in(c + SLOTS)

    def finish_sum(role, side, place, j):
        held, act = helds[role], acts[role]
        total = parts[role][place, side].astype(jnp.float32) + held[side, place].astype(jnp.float32)
        is_head, is_unit, kind = plan.kind(role, j)[:3]

        @pl.when(is_head)
        def _():
            held[side, place] = total.astype(jnp.bfloat16)

        @pl.when(both(is_head, kind == 2))
        def _():
            scores = lax.dot_general(
                held[side, place - 2],
                held[side, place - 1],
                (((1,), (1,)), ((), ())),
                preferred_element_type=jnp.float32,
            ) / (float(HEAD) ** 0.5)
            expo = jnp.exp(scores - jnp.max(scores, axis=-1, keepdims=True))
            probs = (expo / jnp.sum(expo, axis=-1, keepdims=True)).astype(jnp.bfloat16)
            mixed = jnp.dot(probs, total.astype(jnp.bfloat16), preferred_element_type=jnp.float32)
            act[side, place] = mixed.astype(jnp.bfloat16)

        @pl.when(is_unit)
        def _():
            act[side, place] = (0.5 * total * (1.0 + lax.erf(total * (0.5**0.5)))).astype(jnp.bfloat16)

    def spread_stage(role, s):
        for side in range(2):
            dist = hops_of(1 - side)
            c = s - base[role] - entry[role] - LAG * (last + dist)
            _, j = split(c)

            @pl.when(both(dist > 0, in_range(c), yields(role, j)))
            def _():
                place = place_of(role, c)
                spread_copy(role, side, place).wait_recv()

                @pl.when(dist < last)
                def _():
                    spread_copy(role, side, place).start()

                if role == 1:
                    back_copy(side, place).start()

    def reduce_stage(role, s):
        if role == 1:
            c_rung = s - base[role] - RUNG

            @pl.when(both(in_range(c_rung), used(1, split(c_rung)[1])))
            def _():
                rung_copy(far_place(c_rung)).wait_recv()

        for side in range(2):
            hops = hops_of(side)
            c = s - base[role] - entry[role] - LAG * hops
            live = both(in_range(c), used(role, split(c)[1]))

            @pl.when(both(live, hops == 0))
            def _():
                reduce_copy(role, side, place_of(role, c), True).start()

            @pl.when(both(live, hops > 0, hops < last))
            def _():
                place, held = place_of(role, c), helds[role]
                reduce_copy(role, side, place, False).wait_recv()
                held[side, place] = (
                    parts[role][place, side].astype(jnp.float32) + held[side, place].astype(jnp.float32)
                ).astype(jnp.bfloat16)
                reduce_copy(role, side, place, False).start()

    def root_stage(role, s):
        side = jnp.where(row == 0, 0, 1)
        c = s - base[role] - entry[role] - LAG * last
        _, j = split(c)

        @pl.when(both(jnp.logical_or(row == 0, row == last), in_range(c), used(role, j)))
        def _():
            place = place_of(role, c)
            for which in range(2):

                @pl.when(side == which)
                def _():
                    reduce_copy(role, which, place, False).wait_recv()

            finish_sum(role, side, place, j)

            @pl.when(yields(role, j))
            def _():
                for which in range(2):

                    @pl.when(side == which)
                    def _():
                        spread_copy(role, which, place).start()
                        if role == 1:
                            back_copy(which, place).start()

    def down_stage(half, s):
        c = s - base[0] - line - 2 * RUNG * half

        @pl.when(in_range(c))
        def _():
            image, j = split(c)
            slot = lax.rem(c, SLOTS)
            if half == 0:

                @pl.when(j == 0)
                def _():
                    acc[image] = jnp.zeros((cols, patches, width), jnp.float32)

            @pl.when(yields(half, j))
            def _():
                place, source = place_of(half, c), (act_near, back)[half]
                for side in range(2):
                    if half == 1:
                        back_copy(side, place).wait_recv()
                    out_copy(wdown_ref, half, side, slot, 0).wait()
                lhs = jnp.concatenate([source[0, place], source[1, place]], axis=1)
                acc[image] += jnp.dot(lhs, dbuf[slot, half], preferred_element_type=jnp.float32).reshape(
                    cols, patches, width
                )

            @pl.when(c + SLOTS < count)
            def _():
                fetch_out(half, c + SLOTS)

    def pair_copy(image):
        return remote(
            pair_out.at[image], pair_in.at[image], pair_sem.at[0, image], pair_sem.at[1, image], col=partner
        )

    def cross_copy(image, step):
        return remote(
            cross_out.at[image, step],
            cross_in.at[image, step],
            cross_sem.at[0, image, step],
            cross_sem.at[1, image, step],
            col=2 * chip_at(step) + core,
        )

    def pass_copy(image):
        return remote(
            out_ref.at[image], inbox.at[image], pass_sem.at[0, image], pass_sem.at[1, image], section=1 - section
        )

    def event(s, first):
        since = s - first
        return both(in_range(since), lax.rem(since, per_image) == 0), lax.div(since, per_image)

    def close_stage(s):
        ending = base[0] + closing
        at_end, image_end = event(s, ending)

        @pl.when(at_end)
        def _():
            for step in range(chips):
                theirs = 2 * chip_at(step) + (1 - core)
                pair_out[image_end, step] = acc[image_end, theirs].astype(jnp.bfloat16)
            pair_copy(image_end).start()

        at_pair, image_pair = event(s, ending + PAIR_LAG)

        @pl.when(at_pair)
        def _():
            pair_copy(image_pair).wait_recv()
            for step in range(1, chips):
                cross_out[image_pair, step] = (
                    acc[image_pair, 2 * chip_at(step) + core] + pair_in[image_pair, step].astype(jnp.float32)
                ).astype(jnp.bfloat16)
                cross_copy(image_pair, step).start()

        at_cross, image_cross = event(s, ending + PAIR_LAG + CROSS_LAG)

        @pl.when(at_cross)
        def _():
            total = acc[image_cross, col] + pair_in[image_cross, 0].astype(jnp.float32)
            for step in range(1, chips):
                cross_copy(image_cross, step).wait_recv()
                total = total + cross_in[image_cross, step].astype(jnp.float32)
            out_ref[image_cross] = (inbox[image_cross].astype(jnp.float32) + total).astype(jnp.bfloat16)

            @pl.when(section == 0)
            def _():
                pass_copy(image_cross).start()

    def open_stage(s):
        at_pass, image_pass = event(s, arrive)

        @pl.when(at_pass)
        def _():
            pass_copy(image_pass).wait_recv()
            measure(image_pass)

        at_stat, image_stat = event(s, arrive + STAT_LAG)

        @pl.when(at_stat)
        def _():
            normalize(image_stat)

        at_relay, image_relay = event(s, arrive + STAT_LAG + RELAY_LAG)

        @pl.when(at_relay)
        def _():
            relay(image_relay)

        at_full, image_full = event(s, second - 1)

        @pl.when(at_full)
        def _():
            gathered(image_full)

    for c in range(SLOTS):
        fetch_in(jnp.int32(c))
        for half in range(2):
            fetch_out(half, jnp.int32(c))

    @pl.when(section == 0)
    def _():
        inbox[...] = x_ref[...]
        for image in range(images):
            measure(image)
        for image in range(images):
            normalize(image)
        relay(0)
        gathered(0)

    def step(at, carry):
        s = at - 1
        for role in range(2):
            spread_stage(role, s)
        for role in range(2):
            reduce_stage(role, s)
        for role in range(2):
            root_stage(role, s)

        @pl.when(section == 0)
        def _():
            for image in range(1, images):

                @pl.when(s == image * per_image - per_image // 2)
                def _():
                    relay(image)

                @pl.when(s == image * per_image - 1)
                def _():
                    gathered(image)

        @pl.when(section == 1)
        def _():
            open_stage(s)

        c_next = s - base[0] + 1

        @pl.when(in_range(c_next))
        def _():
            project(c_next)

        for half in range(2):
            down_stage(half, s)
        close_stage(s)
        return carry

    steps = second + count - per_image + closing + PAIR_LAG + CROSS_LAG + 2
    lax.fori_loop(0, steps, step, 0)

    def drain(c, carry):
        _, j = split(c)
        for role in range(2):
            for side in range(2):

                @pl.when(both(used(role, j), hops_of(side) < last))
                def _():
                    reduce_copy(role, side, place_of(role, c), False).wait_send()

                @pl.when(both(yields(role, j), hops_of(1 - side) < last))
                def _():
                    spread_copy(role, side, place_of(role, c)).wait_send()

                if role == 1:

                    @pl.when(yields(role, j))
                    def _():
                        back_copy(side, far_place(c)).wait_send()

        @pl.when(used(1, j))
        def _():
            rung_copy(far_place(c)).wait_send()

        return carry

    lax.fori_loop(0, count, drain, 0)

    for image in range(images):
        for step in range(1, rows):
            stat_copy(image, step).wait_send()
        for step in range(chips):
            gather_pair(image, step).wait_send()
            if step:
                gather_cross(image, step).wait_send()
                cross_copy(image, step).wait_send()
        pair_copy(image).wait_send()

        @pl.when(section == 0)
        def _():
            pass_copy(image).wait_send()


def fused_layers(x, weights):
    gain, wq, wk, wv, wup, wout, wdown = weights
    plan = plan_of(x, wq, wup)
    images, patches, width = x.shape
    rows, cols = plan.rows, plan.cols
    chips = cols // 2
    near, far = images * plan.slots(), images * (plan.used()[1] + 1)
    total_rows = patches * cols
    bf16, f32 = jnp.bfloat16, jnp.float32
    dma = pltpu.SemaphoreType.DMA
    vmem = pl.BlockSpec(memory_space=pltpu.VMEM)
    hbm = pl.BlockSpec(memory_space=pl.ANY)
    return pl.pallas_call(
        functools.partial(layers_kernel, plan),
        out_shape=jax.ShapeDtypeStruct(x.shape, bf16),
        in_specs=[vmem, vmem] + [hbm] * 6,
        out_specs=vmem,
        scratch_shapes=[
            pltpu.VMEM(x.shape, bf16),
            pltpu.VMEM((images, rows, patches, 128), f32),
            pltpu.VMEM((images, cols, patches, width), bf16),
            pltpu.VMEM((near, 2, total_rows, HEAD), bf16),
            pltpu.VMEM((far, 2, total_rows, HEAD), bf16),
            pltpu.VMEM((2, near, total_rows, HEAD), bf16),
            pltpu.VMEM((2, far, total_rows, HEAD), bf16),
            pltpu.VMEM((2, near, total_rows, HEAD), bf16),
            pltpu.VMEM((2, far, total_rows, HEAD), bf16),
            pltpu.VMEM((far, 2, total_rows, HEAD), bf16),
            pltpu.VMEM((2, far, total_rows, HEAD), bf16),
            pltpu.VMEM((SLOTS, 2, width, 2 * HEAD), bf16),
            pltpu.VMEM((SLOTS, 2, 2 * HEAD, width), bf16),
            pltpu.VMEM((images, cols, patches, width), f32),
            pltpu.VMEM((images, chips, patches, width), bf16),
            pltpu.VMEM((images, chips, patches, width), bf16),
            pltpu.VMEM((images, chips, patches, width), bf16),
            pltpu.VMEM((images, chips, patches, width), bf16),
            dma((2, images, rows)),
            dma((2, 2, images, chips)),
            dma((SLOTS, 2, 2)),
            dma((SLOTS, 2, 2)),
            dma((2, 2, near)),
            dma((2, 2, far)),
            dma((2, 2, near)),
            dma((2, 2, far)),
            dma((2, far)),
            dma((2, 2, far)),
            dma((2, images)),
            dma((2, images, chips)),
            dma((2, images)),
        ],
        compiler_params=pltpu.CompilerParams(
            collective_id=0, has_side_effects=True, vmem_limit_bytes=VMEM_BYTES
        ),
    )(x, gain[None], wq, wk, wv, wup, wout, wdown)


def fits(x, wq, wup):
    rows, cols = lax.axis_size("row"), lax.axis_size("col")
    if lax.axis_size("section") != 2 or rows < 2 or cols % 2 or x.shape[1] % 16:
        return False
    if wq.shape[1] % (2 * HEAD) or wup.shape[1] % (2 * HEAD):
        return False
    plan = plan_of(x, wq, wup)
    if not plan.heads[1] or not plan.units[1] or plan.slots() < 12 or plan.quota(0) < 1:
        return False
    dealt = plan.quota(1) <= plan.quota(0) and plan.heads[0] * plan.quota(0) >= plan.units[0]
    return dealt and plan.used()[0] < plan.slots()


def passed_along(value, axis, steps):
    count = lax.axis_size(axis)
    first, last = (max(0, -steps), min(count, count - steps))
    return lax.ppermute(value, axis, [(source, source + steps) for source in range(first, last)])


def layer(x, weights):
    gain, wq, wk, wv, wup, wout, wdown = weights
    xf = x.astype(jnp.float32)
    sums, squares = lax.psum((jnp.sum(xf, axis=-1), jnp.sum(xf * xf, axis=-1)), "row")
    mean = (sums / D)[..., None]
    var = jnp.maximum((squares / D)[..., None] - mean * mean, 0.0)
    normed = ((xf - mean) * lax.rsqrt(var + EPS) * gain).astype(jnp.bfloat16)
    gathered = lax.all_gather(normed, "col", axis=1, tiled=True)
    part_q = jnp.dot(gathered, wq, preferred_element_type=jnp.float32)
    part_k = jnp.dot(gathered, wk, preferred_element_type=jnp.float32)
    part_v = jnp.dot(gathered, wv, preferred_element_type=jnp.float32)
    part_m = jnp.dot(gathered, wup, preferred_element_type=jnp.float32)
    query, keyed, valued, pre = (
        lax.psum_scatter(
            part_q.astype(jnp.bfloat16), "row", scatter_dimension=1, tiled=True
        ).astype(jnp.float32),
        lax.psum_scatter(
            part_k.astype(jnp.bfloat16), "row", scatter_dimension=1, tiled=True
        ).astype(jnp.float32),
        lax.psum_scatter(
            part_v.astype(jnp.bfloat16), "row", scatter_dimension=1, tiled=True
        ).astype(jnp.float32),
        lax.psum_scatter(
            part_m.astype(jnp.bfloat16), "row", scatter_dimension=1, tiled=True
        ).astype(jnp.float32),
    )
    act = jax.nn.gelu(pre, approximate=False).astype(jnp.bfloat16)
    query = query.astype(jnp.bfloat16)
    keyed = keyed.astype(jnp.bfloat16)
    valued = valued.astype(jnp.bfloat16)
    all_keys, all_values = (
        lax.all_gather(keyed, "row", axis=1, tiled=True),
        lax.all_gather(valued, "row", axis=1, tiled=True),
    )
    head_dim = D // HEADS
    local_heads = query.shape[2] // head_dim
    images = query.shape[0]
    qh = query.reshape(images, query.shape[1], local_heads, head_dim)
    kh = all_keys.reshape(images, all_keys.shape[1], local_heads, head_dim)
    vh = all_values.reshape(images, all_values.shape[1], local_heads, head_dim)
    scores = jnp.einsum("bqhd,bkhd->bhqk", qh, kh, preferred_element_type=jnp.float32) / jnp.sqrt(
        jnp.float32(head_dim)
    )
    scores = scores - jnp.max(scores, axis=-1, keepdims=True)
    expo = jnp.exp(scores)
    probs = (expo / jnp.sum(expo, axis=-1, keepdims=True)).astype(jnp.bfloat16)
    attn = jnp.einsum("bhqk,bkhd->bqhd", probs, vh, preferred_element_type=jnp.float32)
    attn = attn.reshape(query.shape).astype(jnp.bfloat16)
    attn_full, act_full = (
        lax.all_gather(attn, "row", axis=1, tiled=True),
        lax.all_gather(act, "row", axis=1, tiled=True),
    )
    mixed = jnp.dot(attn_full, wout, preferred_element_type=jnp.float32) + jnp.dot(
        act_full, wdown, preferred_element_type=jnp.float32
    )
    summed = lax.psum_scatter(
        mixed.astype(jnp.bfloat16), "col", scatter_dimension=1, tiled=True
    ).astype(jnp.float32)
    return (xf + summed).astype(jnp.bfloat16)


def pass_on(output):
    return passed_along(output, "section", 1)


def local(tokens, ln_gain, w_query, w_key, w_value, w_up, w_out, w_down):
    weights = (ln_gain[0], w_query[0], w_key[0], w_value[0], w_up[0], w_out[0], w_down[0])
    section = lax.axis_index("section")
    sections = lax.axis_size("section")
    if fits(tokens, w_query[0], w_up[0]):
        return fused_layers(tokens, weights)[None]
    result = jnp.zeros_like(tokens)
    images = tokens.shape[0]
    ticks = images + sections - 1
    inbox = jnp.zeros_like(tokens[:1])
    positions = jnp.arange(images, dtype=jnp.int32)
    for tick in range(ticks):
        fresh = tokens[min(tick, images - 1) : min(tick, images - 1) + 1]
        current = jnp.where(section == 0, fresh, inbox)
        output = layer(current, weights)
        slot = tick - section
        result = jnp.where((positions == slot)[:, None, None], output, result)
        if tick + 1 < ticks:
            inbox = pass_on(output)
    return result[None]


def solution(mesh):
    return jax.shard_map(
        local,
        mesh=mesh,
        in_specs=(
            P(None, "col", "row"),
            P("section", "row"),
            P("section", "row", "col"),
            P("section", "row", "col"),
            P("section", "row", "col"),
            P("section", "row", "col"),
            P("section", "col", "row"),
            P("section", "col", "row"),
        ),
        out_specs=P("section", None, "col", "row"),
        check_vma=False,
    )
```

```python
import functools
from typing import NamedTuple

import jax
import jax.numpy as jnp
from jax import lax
from jax.experimental import pallas as pl
from jax.experimental.pallas import tpu as pltpu
from jax.sharding import PartitionSpec as P

D = 6144
HEADS = 48
HEAD = D // HEADS


EPS = 1e-06
MESH = pl.DeviceIdType.MESH
VMEM_BYTES = 67043328
LAG = 2
RUNG = 2
SLOTS = 3
PAIR_LAG = 2
CROSS_LAG = 3
PASS_LAG = 2
STAT_LAG = 2
RELAY_LAG = 2
GATHER_LAG = 1


class Plan(NamedTuple):
    rows: int
    cols: int
    images: int
    heads: tuple
    units: tuple

    def slots(self):
        return 3 * self.heads[0] + self.units[0]

    def group(self):
        return -(-self.slots() // self.heads[0])

    def quota(self, half):
        return -(-self.units[1] // self.heads[0]) if half else self.group() - 3

    def kind(self, half, j):
        group, pos = lax.div(j, self.group()), lax.rem(j, self.group())
        unit = group * self.quota(half) + pos - 3
        is_head = both(pos < 3, group < self.heads[half])
        is_unit = both(pos >= 3, pos < 3 + self.quota(half), unit < self.units[half])
        return is_head, is_unit, pos, group, unit, group * (3 + self.quota(half)) + pos

    def used(self):
        groups, quota = self.heads[0], self.quota(1)
        used = [(g, p) for g in range(self.heads[1]) for p in range(3)]
        used += [(u // quota, 3 + u % quota) for u in range(self.units[1])]
        return max(g * self.group() + p for g, p in used), max(g * (3 + quota) + p for g, p in used)


def plan_of(x, wq, wup):
    heads = wq.shape[1] // HEAD // 2
    units = wup.shape[1] // HEAD // 2
    far_heads = heads // 2
    far_units = units // 2
    return Plan(
        lax.axis_size("row"),
        lax.axis_size("col"),
        x.shape[0],
        (heads - far_heads, far_heads),
        (units - far_units, far_units),
    )


def greet_peers(axes):
    barrier = pltpu.get_barrier_semaphore()
    total = 0
    for axis, count in axes:
        me = lax.axis_index(axis)
        for step in range(1, count):
            pl.semaphore_signal(
                barrier, inc=1, device_id={axis: lax.rem(me + step, count)}, device_id_type=MESH
            )
            total += 1
    pl.semaphore_wait(barrier, total)


def both(first, *rest):
    for other in rest:
        first = jnp.logical_and(first, other)
    return first


def layers_kernel(
    plan,
    x_ref,
    gain_ref,
    wq_ref,
    wk_ref,
    wv_ref,
    wup_ref,
    wout_ref,
    wdown_ref,
    out_ref,
    inbox,
    stats,
    full,
    part_near,
    part_far,
    held_near,
    held_far,
    act_near,
    act_far,
    away,
    back,
    wbuf,
    dbuf,
    acc,
    pair_out,
    pair_in,
    cross_out,
    cross_in,
    stat_sem,
    gather_sem,
    wsem,
    dsem,
    reduce_near,
    reduce_far,
    spread_near,
    spread_far,
    rung_sem,
    back_sem,
    pair_sem,
    cross_sem,
    pass_sem,
):
    rows, cols, images = plan.rows, plan.cols, plan.images
    last = rows - 1
    per_image, per_far = plan.slots(), plan.used()[1] + 1
    count = images * per_image
    row, col, section = lax.axis_index("row"), lax.axis_index("col"), lax.axis_index("section")
    chips = cols // 2
    chip, core = lax.div(col, 2), lax.rem(col, 2)
    partner = 2 * chip + (1 - core)
    patches, width = x_ref.shape[1], x_ref.shape[2]
    total_rows = patches * cols
    line = 2 * LAG * last
    closing = max(per_image - 1, plan.used()[0] + 2 * RUNG) + line
    passed = closing + PAIR_LAG + CROSS_LAG
    arrive = passed + PASS_LAG
    second = arrive + STAT_LAG + RELAY_LAG + GATHER_LAG + 1
    base = (section * second, (1 - section) * second)
    entry = (0, RUNG)
    parts, helds, acts = (part_near, part_far), (held_near, held_far), (act_near, act_far)
    reduce_sems, spread_sems = (reduce_near, reduce_far), (spread_near, spread_far)
    greet_peers((("row", rows), ("col", cols), ("section", 2)))

    def remote(src, dst, send, recv, **where):
        return pltpu.make_async_remote_copy(
            src_ref=src, dst_ref=dst, send_sem=send, recv_sem=recv, device_id=where, device_id_type=MESH
        )

    def split(c):
        return lax.div(c, per_image), lax.rem(c, per_image)

    def far_place(c):
        image, j = split(c)
        return image * per_far + plan.kind(1, j)[5]

    def place_of(role, c):
        return c if role == 0 else far_place(c)

    def in_range(c):
        return both(c >= 0, c < count)

    def used(role, j):
        is_head, is_unit = plan.kind(role, j)[:2]
        return jnp.logical_or(is_head, is_unit)

    def yields(role, j):
        is_head, is_unit, pos = plan.kind(role, j)[:3]
        return jnp.logical_or(both(is_head, pos == 2), is_unit)

    def chip_at(step):
        return lax.rem(chip + step, chips)

    def chip_behind(step):
        return lax.rem(chip + chips - step, chips)

    def gather_cross(image, step):
        place = full.at[image, col]
        return remote(
            place,
            place,
            gather_sem.at[0, 0, image, step],
            gather_sem.at[0, 1, image, step],
            col=2 * chip_at(step) + core,
        )

    def gather_pair(image, step):
        place = full.at[image, 2 * chip_behind(step) + core]
        return remote(
            place, place, gather_sem.at[1, 0, image, step], gather_sem.at[1, 1, image, step], col=partner
        )

    def stat_copy(image, step):
        return remote(
            stats.at[image, 0],
            stats.at[image, step],
            stat_sem.at[0, image, step],
            stat_sem.at[1, image, step],
            row=lax.rem(row + step, rows),
        )

    def measure(image):
        xf = inbox[image].astype(jnp.float32)
        total = jnp.sum(xf, axis=-1, keepdims=True)
        square = jnp.sum(xf * xf, axis=-1, keepdims=True)
        lane = lax.broadcasted_iota(jnp.int32, (patches, 128), 1)
        stats[image, 0] = jnp.where(lane < 64, total, square)
        for step in range(1, rows):
            stat_copy(image, step).start()

    def normalize(image):
        sums = stats[image, 0]
        for step in range(1, rows):
            stat_copy(image, step).wait_recv()
            sums = sums + stats[image, step]
        mean = sums[:, 0:1] / D
        var = jnp.maximum(sums[:, 64:65] / D - mean * mean, 0.0)
        xf = inbox[image].astype(jnp.float32)
        full[image, col] = ((xf - mean) * lax.rsqrt(var + EPS) * gain_ref[...]).astype(jnp.bfloat16)
        for step in range(1, chips):
            gather_cross(image, step).start()
        gather_pair(image, 0).start()

    def relay(image):
        for step in range(1, chips):
            gather_cross(image, step).wait_recv()
            gather_pair(image, step).start()

    def gathered(image):
        for step in range(chips):
            gather_pair(image, step).wait_recv()

    def head_base(half, side):
        return side * plan.heads[0] if half == 0 else 2 * plan.heads[0] + side * plan.heads[1]

    def unit_base(half, side):
        return side * plan.units[0] if half == 0 else 2 * plan.units[0] + side * plan.units[1]

    def in_copy(ref, half, side, slot, block):
        start = pl.multiple_of(block * HEAD, HEAD)
        return pltpu.make_async_copy(
            ref.at[:, pl.ds(start, HEAD)],
            wbuf.at[slot, half, :, pl.ds(side * HEAD, HEAD)],
            wsem.at[slot, half, side],
        )

    def out_copy(ref, half, side, slot, block):
        start = pl.multiple_of(block * HEAD, HEAD)
        return pltpu.make_async_copy(
            ref.at[pl.ds(start, HEAD), :],
            dbuf.at[slot, half, pl.ds(side * HEAD, HEAD), :],
            dsem.at[slot, half, side],
        )

    def fetch_in(c):
        _, j = split(c)
        slot = lax.rem(c, SLOTS)
        for half in range(2):
            is_head, is_unit, kind, head, unit, _ = plan.kind(half, j)
            for index, ref in enumerate((wq_ref, wk_ref, wv_ref)):

                @pl.when(both(is_head, kind == index))
                def _():
                    for side in range(2):
                        in_copy(ref, half, side, slot, head_base(half, side) + head).start()

            @pl.when(is_unit)
            def _():
                for side in range(2):
                    in_copy(wup_ref, half, side, slot, unit_base(half, side) + unit).start()

    def fetch_out(half, c):
        _, j = split(c)
        slot = lax.rem(c, SLOTS)
        is_head, is_unit, kind, head, unit, _ = plan.kind(half, j)

        @pl.when(both(is_head, kind == 2))
        def _():
            for side in range(2):
                out_copy(wout_ref, half, side, slot, head_base(half, side) + head).start()

        @pl.when(is_unit)
        def _():
            for side in range(2):
                out_copy(wdown_ref, half, side, slot, unit_base(half, side) + unit).start()

    def rung_copy(place):
        return remote(
            away.at[place], part_far.at[place], rung_sem.at[0, place], rung_sem.at[1, place], section=1 - section
        )

    def back_copy(side, place):
        return remote(
            act_far.at[side, place],
            back.at[side, place],
            back_sem.at[0, side, place],
            back_sem.at[1, side, place],
            section=1 - section,
        )

    def toward(side):
        return jnp.minimum(row + 1, last) if side == 1 else jnp.maximum(row - 1, 0)

    def hops_of(side):
        return row if side == 1 else last - row

    def reduce_copy(role, side, place, own_part):
        held, sem = helds[role], reduce_sems[role]
        src = parts[role].at[place, side] if own_part else held.at[side, place]
        return remote(
            src, held.at[side, place], sem.at[0, side, place], sem.at[1, side, place], row=toward(side)
        )

    def spread_copy(role, side, place):
        here, sem = acts[role].at[side, place], spread_sems[role]
        return remote(here, here, sem.at[0, side, place], sem.at[1, side, place], row=toward(1 - side))

    def project(c):
        image, j = split(c)
        slot = lax.rem(c, SLOTS)
        for half in range(2):

            @pl.when(used(half, j))
            def _():
                for side in range(2):
                    in_copy(wup_ref, half, side, slot, 0).wait()
                value = jnp.dot(
                    full[image].reshape(total_rows, width),
                    wbuf[slot, half],
                    preferred_element_type=jnp.float32,
                ).astype(jnp.bfloat16)
                target, place = (part_near, c) if half == 0 else (away, far_place(c))
                target[place, 0] = value[:, :HEAD]
                target[place, 1] = value[:, HEAD:]
                if half == 1:
                    rung_copy(place).start()

        @pl.when(c + SLOTS < count)
        def _():
            fetch_in(c + SLOTS)

    def finish_sum(role, side, place, j):
        held, act = helds[role], acts[role]
        total = parts[role][place, side].astype(jnp.float32) + held[side, place].astype(jnp.float32)
        is_head, is_unit, kind = plan.kind(role, j)[:3]

        @pl.when(is_head)
        def _():
            held[side, place] = total.astype(jnp.bfloat16)

        @pl.when(both(is_head, kind == 2))
        def _():
            scores = lax.dot_general(
                held[side, place - 2],
                held[side, place - 1],
                (((1,), (1,)), ((), ())),
                preferred_element_type=jnp.float32,
            ) / (float(HEAD) ** 0.5)
            expo = jnp.exp(scores - jnp.max(scores, axis=-1, keepdims=True))
            probs = (expo / jnp.sum(expo, axis=-1, keepdims=True)).astype(jnp.bfloat16)
            mixed = jnp.dot(probs, total.astype(jnp.bfloat16), preferred_element_type=jnp.float32)
            act[side, place] = mixed.astype(jnp.bfloat16)

        @pl.when(is_unit)
        def _():
            act[side, place] = (0.5 * total * (1.0 + lax.erf(total * (0.5**0.5)))).astype(jnp.bfloat16)

    def spread_stage(role, s):
        for side in range(2):
            dist = hops_of(1 - side)
            c = s - base[role] - entry[role] - LAG * (last + dist)
            _, j = split(c)

            @pl.when(both(dist > 0, in_range(c), yields(role, j)))
            def _():
                place = place_of(role, c)
                spread_copy(role, side, place).wait_recv()

                @pl.when(dist < last)
                def _():
                    spread_copy(role, side, place).start()

                if role == 1:
                    back_copy(side, place).start()

    def reduce_stage(role, s):
        if role == 1:
            c_rung = s - base[role] - RUNG

            @pl.when(both(in_range(c_rung), used(1, split(c_rung)[1])))
            def _():
                rung_copy(far_place(c_rung)).wait_recv()

        for side in range(2):
            hops = hops_of(side)
            c = s - base[role] - entry[role] - LAG * hops
            live = both(in_range(c), used(role, split(c)[1]))

            @pl.when(both(live, hops == 0))
            def _():
                reduce_copy(role, side, place_of(role, c), True).start()

            @pl.when(both(live, hops > 0, hops < last))
            def _():
                place, held = place_of(role, c), helds[role]
                reduce_copy(role, side, place, False).wait_recv()
                held[side, place] = (
                    parts[role][place, side].astype(jnp.float32) + held[side, place].astype(jnp.float32)
                ).astype(jnp.bfloat16)
                reduce_copy(role, side, place, False).start()

    def root_stage(role, s):
        side = jnp.where(row == 0, 0, 1)
        c = s - base[role] - entry[role] - LAG * last
        _, j = split(c)

        @pl.when(both(jnp.logical_or(row == 0, row == last), in_range(c), used(role, j)))
        def _():
            place = place_of(role, c)
            for which in range(2):

                @pl.when(side == which)
                def _():
                    reduce_copy(role, which, place, False).wait_recv()

            finish_sum(role, side, place, j)

            @pl.when(yields(role, j))
            def _():
                for which in range(2):

                    @pl.when(side == which)
                    def _():
                        spread_copy(role, which, place).start()
                        if role == 1:
                            back_copy(which, place).start()

    def down_stage(half, s):
        c = s - base[0] - line - 2 * RUNG * half

        @pl.when(in_range(c))
        def _():
            image, j = split(c)
            slot = lax.rem(c, SLOTS)
            if half == 0:

                @pl.when(j == 0)
                def _():
                    acc[image] = jnp.zeros((cols, patches, width), jnp.float32)

            @pl.when(yields(half, j))
            def _():
                place, source = place_of(half, c), (act_near, back)[half]
                for side in range(2):
                    if half == 1:
                        back_copy(side, place).wait_recv()
                    out_copy(wdown_ref, half, side, slot, 0).wait()
                lhs = jnp.concatenate([source[0, place], source[1, place]], axis=1)
                acc[image] += jnp.dot(lhs, dbuf[slot, half], preferred_element_type=jnp.float32).reshape(
                    cols, patches, width
                )

            @pl.when(c + SLOTS < count)
            def _():
                fetch_out(half, c + SLOTS)

    def pair_copy(image):
        return remote(
            pair_out.at[image], pair_in.at[image], pair_sem.at[0, image], pair_sem.at[1, image], col=partner
        )

    def cross_copy(image, step):
        return remote(
            cross_out.at[image, step],
            cross_in.at[image, step],
            cross_sem.at[0, image, step],
            cross_sem.at[1, image, step],
            col=2 * chip_at(step) + core,
        )

    def pass_copy(image):
        return remote(
            out_ref.at[image], inbox.at[image], pass_sem.at[0, image], pass_sem.at[1, image], section=1 - section
        )

    def event(s, first):
        since = s - first
        return both(in_range(since), lax.rem(since, per_image) == 0), lax.div(since, per_image)

    def close_stage(s):
        ending = base[0] + closing
        at_end, image_end = event(s, ending)

        @pl.when(at_end)
        def _():
            for step in range(chips):
                theirs = 2 * chip_at(step) + (1 - core)
                pair_out[image_end, step] = acc[image_end, theirs].astype(jnp.bfloat16)
            pair_copy(image_end).start()

        at_pair, image_pair = event(s, ending + PAIR_LAG)

        @pl.when(at_pair)
        def _():
            pair_copy(image_pair).wait_recv()
            for step in range(1, chips):
                cross_out[image_pair, step] = (
                    acc[image_pair, 2 * chip_at(step) + core] + pair_in[image_pair, step].astype(jnp.float32)
                ).astype(jnp.bfloat16)
                cross_copy(image_pair, step).start()

        at_cross, image_cross = event(s, ending + PAIR_LAG + CROSS_LAG)

        @pl.when(at_cross)
        def _():
            total = acc[image_cross, col] + pair_in[image_cross, 0].astype(jnp.float32)
            for step in range(1, chips):
                cross_copy(image_cross, step).wait_recv()
                total = total + cross_in[image_cross, step].astype(jnp.float32)
            out_ref[image_cross] = (inbox[image_cross].astype(jnp.float32) + total).astype(jnp.bfloat16)

            @pl.when(section == 0)
            def _():
                pass_copy(image_cross).start()

    def open_stage(s):
        at_pass, image_pass = event(s, arrive)

        @pl.when(at_pass)
        def _():
            pass_copy(image_pass).wait_recv()
            measure(image_pass)

        at_stat, image_stat = event(s, arrive + STAT_LAG)

        @pl.when(at_stat)
        def _():
            normalize(image_stat)

        at_relay, image_relay = event(s, arrive + STAT_LAG + RELAY_LAG)

        @pl.when(at_relay)
        def _():
            relay(image_relay)

        at_full, image_full = event(s, second - 1)

        @pl.when(at_full)
        def _():
            gathered(image_full)

    for c in range(SLOTS):
        fetch_in(jnp.int32(c))
        for half in range(2):
            fetch_out(half, jnp.int32(c))

    @pl.when(section == 0)
    def _():
        inbox[...] = x_ref[...]
        for image in range(images):
            measure(image)
        for image in range(images):
            normalize(image)
        relay(0)
        gathered(0)

    def step(at, carry):
        s = at - 1
        for role in range(2):
            spread_stage(role, s)
        for role in range(2):
            reduce_stage(role, s)
        for role in range(2):
            root_stage(role, s)

        @pl.when(section == 0)
        def _():
            for image in range(1, images):

                @pl.when(s == image * per_image - per_image // 2)
                def _():
                    relay(image)

                @pl.when(s == image * per_image - 1)
                def _():
                    gathered(image)

        @pl.when(section == 1)
        def _():
            open_stage(s)

        c_next = s - base[0] + 1

        @pl.when(in_range(c_next))
        def _():
            project(c_next)

        for half in range(2):
            down_stage(half, s)
        close_stage(s)
        return carry

    steps = second + count - per_image + closing + PAIR_LAG + CROSS_LAG + 2
    lax.fori_loop(0, steps, step, 0)

    def drain(c, carry):
        _, j = split(c)
        for role in range(2):
            for side in range(2):

                @pl.when(both(used(role, j), hops_of(side) < last))
                def _():
                    reduce_copy(role, side, place_of(role, c), False).wait_send()

                @pl.when(both(yields(role, j), hops_of(1 - side) < last))
                def _():
                    spread_copy(role, side, place_of(role, c)).wait_send()

                if role == 1:

                    @pl.when(yields(role, j))
                    def _():
                        back_copy(side, far_place(c)).wait_send()

        @pl.when(used(1, j))
        def _():
            rung_copy(far_place(c)).wait_send()

        return carry

    lax.fori_loop(0, count, drain, 0)

    for image in range(images):
        for step in range(1, rows):
            stat_copy(image, step).wait_send()
        for step in range(chips):
            gather_pair(image, step).wait_send()
            if step:
                gather_cross(image, step).wait_send()
                cross_copy(image, step).wait_send()
        pair_copy(image).wait_send()

        @pl.when(section == 0)
        def _():
            pass_copy(image).wait_send()


def fused_layers(x, weights):
    gain, wq, wk, wv, wup, wout, wdown = weights
    plan = plan_of(x, wq, wup)
    images, patches, width = x.shape
    rows, cols = plan.rows, plan.cols
    chips = cols // 2
    near, far = images * plan.slots(), images * (plan.used()[1] + 1)
    total_rows = patches * cols
    bf16, f32 = jnp.bfloat16, jnp.float32
    dma = pltpu.SemaphoreType.DMA
    vmem = pl.BlockSpec(memory_space=pltpu.VMEM)
    hbm = pl.BlockSpec(memory_space=pl.ANY)
    return pl.pallas_call(
        functools.partial(layers_kernel, plan),
        out_shape=jax.ShapeDtypeStruct(x.shape, bf16),
        in_specs=[vmem, vmem] + [hbm] * 6,
        out_specs=vmem,
        scratch_shapes=[
            pltpu.VMEM(x.shape, bf16),
            pltpu.VMEM((images, rows, patches, 128), f32),
            pltpu.VMEM((images, cols, patches, width), bf16),
            pltpu.VMEM((near, 2, total_rows, HEAD), bf16),
            pltpu.VMEM((far, 2, total_rows, HEAD), bf16),
            pltpu.VMEM((2, near, total_rows, HEAD), bf16),
            pltpu.VMEM((2, far, total_rows, HEAD), bf16),
            pltpu.VMEM((2, near, total_rows, HEAD), bf16),
            pltpu.VMEM((2, far, total_rows, HEAD), bf16),
            pltpu.VMEM((far, 2, total_rows, HEAD), bf16),
            pltpu.VMEM((2, far, total_rows, HEAD), bf16),
            pltpu.VMEM((SLOTS, 2, width, 2 * HEAD), bf16),
            pltpu.VMEM((SLOTS, 2, 2 * HEAD, width), bf16),
            pltpu.VMEM((images, cols, patches, width), f32),
            pltpu.VMEM((images, chips, patches, width), bf16),
            pltpu.VMEM((images, chips, patches, width), bf16),
            pltpu.VMEM((images, chips, patches, width), bf16),
            pltpu.VMEM((images, chips, patches, width), bf16),
            dma((2, images, rows)),
            dma((2, 2, images, chips)),
            dma((SLOTS, 2, 2)),
            dma((SLOTS, 2, 2)),
            dma((2, 2, near)),
            dma((2, 2, far)),
            dma((2, 2, near)),
            dma((2, 2, far)),
            dma((2, far)),
            dma((2, 2, far)),
            dma((2, images)),
            dma((2, images, chips)),
            dma((2, images)),
        ],
        compiler_params=pltpu.CompilerParams(
            collective_id=0, has_side_effects=True, vmem_limit_bytes=VMEM_BYTES
        ),
    )(x, gain[None], wq, wk, wv, wup, wout, wdown)


def fits(x, wq, wup):
    rows, cols = lax.axis_size("row"), lax.axis_size("col")
    if lax.axis_size("section") != 2 or rows < 2 or cols % 2 or x.shape[1] % 16:
        return False
    if wq.shape[1] % (2 * HEAD) or wup.shape[1] % (2 * HEAD):
        return False
    plan = plan_of(x, wq, wup)
    if not plan.heads[1] or not plan.units[1] or plan.slots() < 12 or plan.quota(0) < 1:
        return False
    dealt = plan.quota(1) <= plan.quota(0) and plan.heads[0] * plan.quota(0) >= plan.units[0]
    return dealt and plan.used()[0] < plan.slots()


def passed_along(value, axis, steps):
    count = lax.axis_size(axis)
    first, last = (max(0, -steps), min(count, count - steps))
    return lax.ppermute(value, axis, [(source, source + steps) for source in range(first, last)])


def layer(x, weights):
    gain, wq, wk, wv, wup, wout, wdown = weights
    xf = x.astype(jnp.float32)
    sums, squares = lax.psum((jnp.sum(xf, axis=-1), jnp.sum(xf * xf, axis=-1)), "row")
    mean = (sums / D)[..., None]
    var = jnp.maximum((squares / D)[..., None] - mean * mean, 0.0)
    normed = ((xf - mean) * lax.rsqrt(var + EPS) * gain).astype(jnp.bfloat16)
    gathered = lax.all_gather(normed, "col", axis=1, tiled=True)
    part_q = jnp.dot(gathered, wq, preferred_element_type=jnp.float32)
    part_k = jnp.dot(gathered, wk, preferred_element_type=jnp.float32)
    part_v = jnp.dot(gathered, wv, preferred_element_type=jnp.float32)
    part_m = jnp.dot(gathered, wup, preferred_element_type=jnp.float32)
    query, keyed, valued, pre = (
        lax.psum_scatter(
            part_q.astype(jnp.bfloat16), "row", scatter_dimension=1, tiled=True
        ).astype(jnp.float32),
        lax.psum_scatter(
            part_k.astype(jnp.bfloat16), "row", scatter_dimension=1, tiled=True
        ).astype(jnp.float32),
        lax.psum_scatter(
            part_v.astype(jnp.bfloat16), "row", scatter_dimension=1, tiled=True
        ).astype(jnp.float32),
        lax.psum_scatter(
            part_m.astype(jnp.bfloat16), "row", scatter_dimension=1, tiled=True
        ).astype(jnp.float32),
    )
    act = jax.nn.gelu(pre, approximate=False).astype(jnp.bfloat16)
    query = query.astype(jnp.bfloat16)
    keyed = keyed.astype(jnp.bfloat16)
    valued = valued.astype(jnp.bfloat16)
    all_keys, all_values = (
        lax.all_gather(keyed, "row", axis=1, tiled=True),
        lax.all_gather(valued, "row", axis=1, tiled=True),
    )
    head_dim = D // HEADS
    local_heads = query.shape[2] // head_dim
    images = query.shape[0]
    qh = query.reshape(images, query.shape[1], local_heads, head_dim)
    kh = all_keys.reshape(images, all_keys.shape[1], local_heads, head_dim)
    vh = all_values.reshape(images, all_values.shape[1], local_heads, head_dim)
    scores = jnp.einsum("bqhd,bkhd->bhqk", qh, kh, preferred_element_type=jnp.float32) / jnp.sqrt(
        jnp.float32(head_dim)
    )
    scores = scores - jnp.max(scores, axis=-1, keepdims=True)
    expo = jnp.exp(scores)
    probs = (expo / jnp.sum(expo, axis=-1, keepdims=True)).astype(jnp.bfloat16)
    attn = jnp.einsum("bhqk,bkhd->bqhd", probs, vh, preferred_element_type=jnp.float32)
    attn = attn.reshape(query.shape).astype(jnp.bfloat16)
    attn_full, act_full = (
        lax.all_gather(attn, "row", axis=1, tiled=True),
        lax.all_gather(act, "row", axis=1, tiled=True),
    )
    mixed = jnp.dot(attn_full, wout, preferred_element_type=jnp.float32) + jnp.dot(
        act_full, wdown, preferred_element_type=jnp.float32
    )
    summed = lax.psum_scatter(
        mixed.astype(jnp.bfloat16), "col", scatter_dimension=1, tiled=True
    ).astype(jnp.float32)
    return (xf + summed).astype(jnp.bfloat16)


def pass_on(output):
    return passed_along(output, "section", 1)


def local(tokens, ln_gain, w_query, w_key, w_value, w_up, w_out, w_down):
    weights = (ln_gain[0], w_query[0], w_key[0], w_value[0], w_up[0], w_out[0], w_down[0])
    section = lax.axis_index("section")
    sections = lax.axis_size("section")
    if fits(tokens, w_query[0], w_up[0]):
        return fused_layers(tokens, weights)[None]
    result = jnp.zeros_like(tokens)
    images = tokens.shape[0]
    ticks = images + sections - 1
    inbox = jnp.zeros_like(tokens[:1])
    positions = jnp.arange(images, dtype=jnp.int32)
    for tick in range(ticks):
        fresh = tokens[min(tick, images - 1) : min(tick, images - 1) + 1]
        current = jnp.where(section == 0, fresh, inbox)
        output = layer(current, weights)
        slot = tick - section
        result = jnp.where((positions == slot)[:, None, None], output, result)
        if tick + 1 < ticks:
            inbox = pass_on(output)
    return result[None]


def solution(mesh):
    return jax.shard_map(
        local,
        mesh=mesh,
        in_specs=(
            P(None, "col", "row"),
            P("section", "row"),
            P("section", "row", "col"),
            P("section", "row", "col"),
            P("section", "row", "col"),
            P("section", "row", "col"),
            P("section", "col", "row"),
            P("section", "col", "row"),
        ),
        out_specs=P("section", None, "col", "row"),
        check_vma=False,
    )
```
